32 devices in a mesh: gx: 4 (over z), gy: 2 (over y), gz: 4 (over x, core).
Axes of the slice: x: 2, y: 2, z: 4, core: 2. Of those that a mesh axis runs over, the one named last changes fastest.
Arguments:
- cell_counts: int32 [16, 4, 16], P('gx', 'gy', 'gz'), may hold values from 64 to 128
- grid_offset: int32 [16, 4, 16, 3, 128], P('gx', 'gy', 'gz'), may hold values from 0 to 14
- fraction: float32 [16, 4, 16, 3, 128], P('gx', 'gy', 'gz'), may hold values from 0 to 1
- species: int32 [16, 4, 16, 128], P('gx', 'gy', 'gz'), may hold values from 0 to 1
- species_density: float32 [2], replicated, may hold values from 0.01 to 0.03
- species_pair: float32 [2], replicated, may hold values from 0.05 to 0.2
- species_embed: float32 [2], replicated, may hold values from 0.5 to 2
- species_charge: float32 [2], replicated, may hold values from -3 to 3
Outputs:
- forces: float32 [16, 4, 16, 3, 128], P('gx', 'gy', 'gz')
- density: float32 [16, 4, 16, 128], P('gx', 'gy', 'gz')
The draws below stay inside these ranges and needn't reach their ends.
Inputs may be any that keep to these rules, and one draw needn't show every extreme that they name: `cell_counts`: slots below the count hold atoms; the others are padding. `grid_offset`: an atom's stencil points lie in its own cell.
All inputs are finite; a program needn't handle non-finite values.
Results may differ from the reference program's by a relative error of at most 0.0003.
Values sent between devices are 32-bit elements; how exact they have to be, the bound alone decides.
A program may use at most 128 MiB of HBM per device.

```python
import math
import jax
import jax.numpy as jnp
from jax import lax

SLOTS = 128
NSPEC = 2
PPC = 16
NX = 16
NY = 4
NZ = 16


def plant(values, key, smallest, top_value):
    longest = values.shape.index(max(values.shape))
    spots = []
    for shift in (0, 1):
        where = [jax.random.randint(jax.random.fold_in(key, axis), (), 0, length) for axis, length in enumerate(values.shape)]
        where[longest] = (where[longest] + shift) % values.shape[longest]
        spots.append(tuple(where))
    return values.at[spots[0]].set(smallest).at[spots[1]].set(top_value)


def block_levels(stream_key, dims, shards, low, largest):
    def one(axis_at, blocks):
        heights = jax.random.uniform(jax.random.fold_in(jax.random.fold_in(stream_key, 6), axis_at), (blocks,), jnp.float32, low / len(shards), largest / len(shards))
        return jnp.repeat(jnp.exp(heights), dims[axis_at] // blocks).reshape((-1,) + (1,) * (len(dims) - axis_at - 1))

    factor_of = one(*shards[0])
    for cut in shards[1:]:
        factor_of = factor_of * one(*cut)
    return factor_of


def noise(stream_key, shape, scale, limit, kind=jnp.bfloat16):
    return jnp.clip(scale * jax.random.normal(stream_key, shape, jnp.float32), -limit, limit).astype(kind)


def setup_inputs(seed: int = 0) -> dict:
    arg_keys = jax.random.split(jax.random.key(seed), 9)
    return {
        "cell_counts": plant(jax.random.randint(arg_keys[0], (NX, NY, NZ), SLOTS // 2, SLOTS + 1), jax.random.fold_in(arg_keys[0], 1), SLOTS // 2, SLOTS).astype(jnp.int32),
        "grid_offset": plant(jax.random.randint(arg_keys[1], (NX, NY, NZ, 3, SLOTS), 0, PPC - 1), jax.random.fold_in(arg_keys[1], 1), 0, (PPC - 1) - 1).astype(jnp.int32),
        "fraction": jnp.clip(1.0 * jax.random.uniform(arg_keys[2], (NX, NY, NZ, 3, SLOTS), jnp.float32) ** block_levels(arg_keys[2], (NX, NY, NZ, 3, SLOTS), ((0, 4), (1, 2), (2, 4)), -0.2, 0.2), 0.0, 1.0),
        "species": plant(jax.random.randint(arg_keys[3], (NX, NY, NZ, SLOTS), 0, NSPEC), jax.random.fold_in(arg_keys[3], 1), 0, NSPEC - 1).astype(jnp.int32),
        "species_density": jnp.clip(jnp.exp(jax.random.uniform(arg_keys[4], (NSPEC,), jnp.float32, math.log(0.01), math.log(0.03))), 0.01, 0.03),
        "species_pair": jnp.clip(jnp.exp(jax.random.uniform(arg_keys[5], (NSPEC,), jnp.float32, math.log(0.05), math.log(0.2))), 0.05, 0.2),
        "species_embed": jnp.clip(jnp.exp(jax.random.uniform(arg_keys[6], (NSPEC,), jnp.float32, math.log(0.5), math.log(2.0))), 0.5, 2.0),
        "species_charge": noise(arg_keys[7], (NSPEC,), 1.0, 3.0, jnp.float32),
    }


EWALD_SPLIT = 0.7
COUPLING = 8.0
HIGHEST_PRECISION = lax.Precision.HIGHEST
neighbour_shifts = [(shift_x, shift_y, shift_z) for shift_x in (-1, 0, 1) for shift_y in (-1, 0, 1) for shift_z in (-1, 0, 1)]

def species_value(species, lookup_table):
    result = jnp.zeros(species.shape, jnp.float32)
    for kind_index in range(NSPEC):
        result = result + jnp.where(species == kind_index, lookup_table[kind_index], 0.0)
    return result

def stencil(offsets, fractions):
    points = lax.broadcasted_iota(jnp.int32, offsets.shape + (PPC,), offsets.ndim)
    lower_point = (points == offsets[..., None]).astype(jnp.float32)
    upper_point = (points == offsets[..., None] + 1).astype(jnp.float32)
    weights = lower_point * (1.0 - fractions[..., None]) + upper_point * fractions[..., None]
    return (weights, upper_point - lower_point)

def spread_cells(charges, weights_x, weights_y, weights_z):
    batch_size, slot_count = charges.shape
    pair_plane = (weights_y[:, :, :, None] * weights_z[:, :, None, :]).reshape(batch_size, slot_count, PPC * PPC)
    return jnp.einsum('bax,bay->bxy', weights_x * charges[:, :, None], pair_plane, precision=HIGHEST_PRECISION)

def outer_plane(first_weights, second_weights):
    batch_size, slot_count, width_count = first_weights.shape
    return (first_weights[:, :, :, None] * second_weights[:, :, None, :]).reshape(batch_size, slot_count, width_count * width_count)

def sample_cells(blocks, charges, weights_x, weights_y, weights_z, slope_x, slope_y, slope_z):
    plain_x = jnp.einsum('bax,bxy->bay', weights_x, blocks, precision=HIGHEST_PRECISION)
    tilted_x = jnp.einsum('bax,bxy->bay', slope_x, blocks, precision=HIGHEST_PRECISION)
    force_x = -charges * lax.optimization_barrier(jnp.sum(tilted_x * outer_plane(weights_y, weights_z), axis=2))
    force_y = -charges * lax.optimization_barrier(jnp.sum(plain_x * outer_plane(slope_y, weights_z), axis=2))
    force_z = -charges * lax.optimization_barrier(jnp.sum(plain_x * outer_plane(weights_y, slope_z), axis=2))
    return jnp.stack([force_x, force_y, force_z], axis=1)

def signed_modes(indices, total):
    return jnp.where(2 * indices >= total, indices - total, indices)

def green_factor(modes_x, modes_y, modes_z, length_x, length_y, length_z):
    wave_x = modes_x.astype(jnp.float32) * (2.0 * math.pi / length_x)
    wave_y = modes_y.astype(jnp.float32) * (2.0 * math.pi / length_y)
    wave_z = modes_z.astype(jnp.float32) * (2.0 * math.pi / length_z)
    squared = wave_x * wave_x + wave_y * wave_y + wave_z * wave_z
    anchor = (modes_x == 0) & (modes_y == 0) & (modes_z == 0)
    safe_square = jnp.where(anchor, 1.0, squared)
    return jnp.where(anchor, 0.0, 4.0 * math.pi * jnp.exp(-squared / (4.0 * EWALD_SPLIT * EWALD_SPLIT)) / safe_square)

def periodic(values):
    widths = [(1, 1), (1, 1), (1, 1)] + [(0, 0)] * (values.ndim - 3)
    return jnp.pad(values, widths, mode='wrap')

def pair_terms(positions, other_positions, shift_triple, not_self):
    shift_vector = jnp.asarray(shift_triple, jnp.float32)
    separation = shift_vector[:, None, None] + other_positions[..., :, None, :] - positions[..., :, :, None]
    squared = lax.optimization_barrier(jnp.sum(separation * separation, axis=-3))
    weight = jnp.maximum(1.0 - squared, 0.0)
    if shift_triple == (0, 0, 0):
        weight = weight * not_self
    return (separation, weight)

def window(rows, shift_triple, cells_y, cells_z):
    return rows[1 + shift_triple[0], 1 + shift_triple[1]:1 + shift_triple[1] + cells_y, 1 + shift_triple[2]:1 + shift_triple[2] + cells_z]

def reference(cell_counts, grid_offset, fraction, species, species_density, species_pair, species_embed, species_charge):
    slot_index = lax.broadcasted_iota(jnp.int32, species.shape, 3)
    alive_mask = (slot_index < cell_counts[..., None]).astype(jnp.float32)
    positions = (grid_offset.astype(jnp.float32) + 0.5 + fraction) / PPC
    density_coef = species_value(species, species_density) * alive_mask
    repulsion = species_value(species, species_pair) * alive_mask
    embedding = species_value(species, species_embed)
    charges = species_value(species, species_charge) * alive_mask
    not_self = (lax.broadcasted_iota(jnp.int32, (SLOTS, SLOTS), 0) != lax.broadcasted_iota(jnp.int32, (SLOTS, SLOTS), 1)).astype(jnp.float32)
    wide_positions = periodic(positions)
    wide_density = periodic(density_coef)
    wide_repulsion = periodic(repulsion)
    row_ids = jnp.arange(NX, dtype=jnp.int32)

    def density_row(row):
        near_pos = lax.dynamic_slice_in_dim(wide_positions, row, 3, 0)
        near_coef = lax.dynamic_slice_in_dim(wide_density, row, 3, 0)
        own = lax.dynamic_index_in_dim(positions, row, 0, keepdims=False)
        total = jnp.zeros((NY, NZ, SLOTS), jnp.float32)
        for shift_triple in neighbour_shifts:
            separation, weight = pair_terms(own, window(near_pos, shift_triple, NY, NZ), shift_triple, not_self)
            total = total + lax.optimization_barrier(jnp.sum(weight * weight * weight * window(near_coef, shift_triple, NY, NZ)[..., None, :], axis=-1))
        return total
    density = lax.map(density_row, row_ids) * alive_mask
    slope_embed = -embedding * alive_mask / (2.0 * jnp.sqrt(1.0 + density))
    wide_slope = periodic(slope_embed)

    def force_row(row):
        near_pos = lax.dynamic_slice_in_dim(wide_positions, row, 3, 0)
        near_coef = lax.dynamic_slice_in_dim(wide_density, row, 3, 0)
        near_rep = lax.dynamic_slice_in_dim(wide_repulsion, row, 3, 0)
        near_slp = lax.dynamic_slice_in_dim(wide_slope, row, 3, 0)
        own = lax.dynamic_index_in_dim(positions, row, 0, keepdims=False)
        own_rep = lax.dynamic_index_in_dim(repulsion, row, 0, keepdims=False)
        own_coef = lax.dynamic_index_in_dim(density_coef, row, 0, keepdims=False)
        own_slope = lax.dynamic_index_in_dim(slope_embed, row, 0, keepdims=False)
        total = jnp.zeros((NY, NZ, 3, SLOTS), jnp.float32)
        for shift_triple in neighbour_shifts:
            separation, weight = pair_terms(own, window(near_pos, shift_triple, NY, NZ), shift_triple, not_self)
            other_coef = window(near_coef, shift_triple, NY, NZ)[..., None, :]
            other_rep = window(near_rep, shift_triple, NY, NZ)[..., None, :]
            other_slope = window(near_slp, shift_triple, NY, NZ)[..., None, :]
            coefficient = -2.0 * own_rep[..., :, None] * other_rep * weight - 3.0 * weight * weight * (own_slope[..., :, None] * other_coef + other_slope * own_coef[..., :, None])
            total = total + 2.0 * lax.optimization_barrier(jnp.sum(coefficient[..., None, :, :] * separation, axis=-1))
        return total
    eam_force = lax.map(force_row, row_ids)
    stencils = [stencil(grid_offset[:, :, :, axis_index, :], fraction[:, :, :, axis_index, :]) for axis_index in range(3)]
    row_cells = NY * NZ

    def spread_row(row_items):
        charge_row, first_row, second_row, third_row = row_items
        return spread_cells(charge_row.reshape(row_cells, SLOTS), first_row.reshape(row_cells, SLOTS, PPC), second_row.reshape(row_cells, SLOTS, PPC), third_row.reshape(row_cells, SLOTS, PPC))
    blocks = lax.map(spread_row, (charges, stencils[0][0], stencils[1][0], stencils[2][0]))
    length_x, length_y, length_z = (NX * PPC, NY * PPC, NZ * PPC)
    charge_grid = blocks.reshape(NX, NY, NZ, PPC, PPC, PPC).transpose(0, 3, 1, 4, 2, 5).reshape(length_x, length_y, length_z)
    modes_x = signed_modes(jnp.arange(length_x, dtype=jnp.int32), length_x)[:, None, None]
    modes_y = signed_modes(jnp.arange(length_y, dtype=jnp.int32), length_y)[None, :, None]
    modes_z = signed_modes(jnp.arange(length_z, dtype=jnp.int32), length_z)[None, None, :]
    factor = green_factor(modes_x, modes_y, modes_z, length_x, length_y, length_z)
    potential = jnp.real(jnp.fft.ifftn(jnp.fft.fftn(charge_grid) * factor)).astype(jnp.float32)
    blocks_back = potential.reshape(NX, PPC, NY, PPC, NZ, PPC).transpose(0, 2, 4, 1, 3, 5).reshape(NX, row_cells, PPC, PPC * PPC)

    def sample_row(row_items):
        block_row, charge_row, first_w, second_w, third_w, first_s, second_s, third_s = row_items

        def shaped(values):
            return values.reshape(row_cells, SLOTS, PPC)
        return sample_cells(block_row, charge_row.reshape(row_cells, SLOTS), shaped(first_w), shaped(second_w), shaped(third_w), shaped(first_s), shaped(second_s), shaped(third_s))
    electric = lax.map(sample_row, (blocks_back, charges, stencils[0][0], stencils[1][0], stencils[2][0], stencils[0][1], stencils[1][1], stencils[2][1]))
    electric = electric.reshape(NX, NY, NZ, 3, SLOTS)
    forces = (eam_force + COUPLING * electric) * alive_mask[:, :, :, None, :]
    return (forces, density)
```

```python
import math

import jax
import jax.numpy as jnp
import numpy as np
from jax import lax
from jax.experimental import pallas as pl
from jax.experimental.pallas import tpu as pltpu
from jax.sharding import PartitionSpec as P

PPC = 16
EWALD_SPLIT = 0.7
COUPLING = 8.0
KF = 32
NT = (((1,), (1,)), ((), ()))
NN = (((1,), (0,)), ((), ()))
VM = pl.BlockSpec(memory_space=pltpu.VMEM)
SM = pl.BlockSpec(memory_space=pltpu.SMEM)


def padded(block, sides, widths):
    for (axis, dim), width in zip(sides, widths):
        count = lax.axis_size(axis)
        forward = [(i, (i + 1) % count) for i in range(count)]
        backward = [(target, source) for source, target in forward]
        low = lax.ppermute(
            lax.slice_in_dim(block, block.shape[dim] - width, None, axis=dim), axis, forward
        )
        high = lax.ppermute(lax.slice_in_dim(block, 0, width, axis=dim), axis, backward)
        block = jnp.concatenate([low, block, high], axis=dim)
    return block


def split2(values):
    high = values.astype(jnp.bfloat16)
    low = (values - high.astype(jnp.float32)).astype(jnp.bfloat16)
    return high, low


def split3(values):
    high = values.astype(jnp.bfloat16).astype(jnp.float32)
    rest = values - high
    mid = rest.astype(jnp.bfloat16).astype(jnp.float32)
    low = (rest - mid).astype(jnp.bfloat16).astype(jnp.float32)
    return high, mid, low


def mm(a, b, dims=NN):
    return lax.dot_general(a, b, dims, preferred_element_type=jnp.float32)


def mm3(a, b, dims=NN):
    return mm(a[0], b[0], dims) + mm(a[0], b[1], dims) + mm(a[1], b[0], dims)


def table(sp, ref):
    result = jnp.zeros(sp.shape, jnp.float32)
    for kind in range(ref.shape[0]):
        result = jnp.where(sp == kind, ref[kind], result)
    return result


def weights_of(off, fr):
    points = lax.broadcasted_iota(jnp.int32, (PPC, off.shape[1]), 0)
    lower = points == off
    upper = points == off + 1
    zero = jnp.zeros((PPC, off.shape[1]), jnp.float32)
    weights = jnp.where(lower, 1.0 - fr, jnp.where(upper, fr, zero))
    slopes = jnp.where(lower, -1.0, jnp.where(upper, 1.0, zero))
    return weights, slopes


def placed(rows, cell, cells):
    parts = []
    if cell:
        parts.append(jnp.zeros((cell * PPC, rows.shape[1]), jnp.float32))
    parts.append(rows)
    if cell < cells - 1:
        parts.append(jnp.zeros(((cells - 1 - cell) * PPC, rows.shape[1]), jnp.float32))
    return jnp.concatenate(parts, axis=0)


def spread_kernel(cnt, off, fr, sp, tden, tpair, temb, tchg, s_ref, pk_ref):
    nx, ny, nz, _, slots = fr.shape

    def body(cx, carry):
        total = jnp.zeros((PPC * PPC, ny * nz * PPC), jnp.float32)
        for cy in range(ny):
            for cz in range(nz):
                cell = cy * nz + cz
                o = off[cx, cy, cz]
                f = fr[cx, cy, cz]
                kind = sp[cx, cy, cz : cz + 1, :]
                lane = lax.broadcasted_iota(jnp.int32, (1, slots), 1)
                alive = (lane < cnt[(cx * ny + cy) * nz + cz]).astype(jnp.float32)
                charge = table(kind, tchg) * alive
                pos = (o.astype(jnp.float32) + 0.5 + f) / PPC
                zero = jnp.zeros((1, slots), jnp.float32)
                pk_ref[cx, cy, :, cz * slots : (cz + 1) * slots] = jnp.concatenate(
                    [
                        pos,
                        table(kind, tden) * alive,
                        table(kind, tpair) * alive,
                        alive,
                        table(kind, temb),
                        zero,
                    ],
                    axis=0,
                )
                wx, _ = weights_of(o[0:1], f[0:1])
                wy, _ = weights_of(o[1:2], f[1:2])
                wz, _ = weights_of(o[2:3], f[2:3])
                wx = wx * charge
                plane = (wy[:, None, :] * wx[None, :, :]).reshape(PPC * PPC, slots)
                ph, pw = split2(plane)
                zh, zw = split2(placed(wz, cell, ny * nz))
                total = total + mm(
                    jnp.concatenate([ph, pw], axis=1), jnp.concatenate([zh, zh], axis=1), NT
                )
                total = total + mm(ph, zw, NT)
        s_ref[:, pl.ds(pl.multiple_of(cx * PPC, PPC), PPC), :] = total.reshape(
            PPC, PPC, ny * nz * PPC
        )
        return carry

    lax.fori_loop(0, nx, body, 0)


def xmodes_kernel(direct, r_ref, qh, ql, h_ref):
    gx, ys, xs, lanes = r_ref.shape
    q = (qh[...], ql[...])
    for y in range(ys):
        data = r_ref[:, y].reshape(gx * xs, lanes)
        out = mm3(q, split2(data))
        if direct:
            h_ref[:, y] = out.reshape(h_ref.shape[0], h_ref.shape[2], lanes)
        else:
            h_ref[y] = out


def xback_kernel(direct, h_ref, qh, ql, p_ref):
    gx, ys, xs, lanes = p_ref.shape
    q = (qh[...], ql[...])
    for y in range(ys):
        data = h_ref[:, y].reshape(gx * xs, lanes) if direct else h_ref[y]
        out = mm3(q, split2(data))
        p_ref[:, y] = out.reshape(gx, xs, lanes)


def plane_kernel(t_ref, wh, wl, kh, kl, green, o_ref):
    groups, gz, sub, lanes = t_ref.shape
    rows = groups * sub
    lz = green.shape[1]
    ny = wh.shape[1] // lz
    data = jnp.concatenate([t_ref[:, g].reshape(rows, lanes) for g in range(gz)], axis=1)
    u = mm3(split2(data), (wh[...], wl[...]))
    u = jnp.concatenate([u[:, c * lz : (c + 1) * lz] for c in range(ny)], axis=0)
    k = (kh[...], kl[...])
    v = mm3(k, split2(u)) * green[...]
    u = mm3(k, split2(v))
    u = jnp.concatenate([u[c * rows : (c + 1) * rows] for c in range(ny)], axis=1)
    out = mm3(split2(u), (wh[...], wl[...]), NT)
    for g in range(gz):
        o_ref[:, g] = out[:, g * lanes : (g + 1) * lanes].reshape(groups, sub, lanes)


def sample_kernel(cnt, off, fr, sp, tchg, phi_ref, eam, out_ref):
    nx, ny, nz, _, slots = fr.shape

    def body(cx, carry):
        phi = phi_ref[:, pl.ds(pl.multiple_of(cx * PPC, PPC), PPC), :].reshape(
            PPC * PPC, ny * nz * PPC
        )
        ph, pw = split2(phi)
        both = jnp.concatenate([ph, pw], axis=1)
        for cy in range(ny):
            for cz in range(nz):
                cell = cy * nz + cz
                o = off[cx, cy, cz]
                f = fr[cx, cy, cz]
                kind = sp[cx, cy, cz : cz + 1, :]
                lane = lax.broadcasted_iota(jnp.int32, (1, slots), 1)
                alive = (lane < cnt[(cx * ny + cy) * nz + cz]).astype(jnp.float32)
                charge = table(kind, tchg) * alive
                wx, sx = weights_of(o[0:1], f[0:1])
                wy, sy = weights_of(o[1:2], f[1:2])
                wz, sz = weights_of(o[2:3], f[2:3])
                zh, zw = split2(placed(wz, cell, ny * nz))
                sh = placed(sz, cell, ny * nz).astype(jnp.bfloat16)
                right = jnp.concatenate([zh, sh], axis=1)
                g = mm(both, jnp.concatenate([right, right], axis=0))
                gw = g[:, :slots] + mm(ph, zw)
                gs = g[:, slots:]
                fx = jnp.zeros((PPC, slots), jnp.float32)
                fy = jnp.zeros((PPC, slots), jnp.float32)
                fz = jnp.zeros((PPC, slots), jnp.float32)
                for y in range(PPC):
                    a = gw[y * PPC : (y + 1) * PPC]
                    b = gs[y * PPC : (y + 1) * PPC]
                    fx = fx + wy[y : y + 1] * a
                    fy = fy + sy[y : y + 1] * a
                    fz = fz + wy[y : y + 1] * b
                field = jnp.concatenate(
                    [
                        jnp.sum(sx * fx, axis=0, keepdims=True),
                        jnp.sum(wx * fy, axis=0, keepdims=True),
                        jnp.sum(wx * fz, axis=0, keepdims=True),
                    ],
                    axis=0,
                )
                out_ref[cx, cy, cz] = (eam[cx, cy, cz] - COUPLING * charge * field) * alive
        return carry

    lax.fori_loop(0, nx, body, 0)


def centred(ext, ex, ey, first_z, lanes, dims):
    nx, ny, nz = dims
    slots_iota = lax.broadcasted_iota(jnp.int32, (3, lanes), 1)
    row = lax.broadcasted_iota(jnp.int32, (3, lanes), 0)
    cell_z = (slots_iota // 128).astype(jnp.float32) + (
        jnp.asarray(first_z, jnp.int32).astype(jnp.float32) - (1.0 + nz / 2)
    )
    cell_x = jnp.asarray(ex, jnp.int32).astype(jnp.float32) - (1.0 + nx / 2)
    cell_y = jnp.asarray(ey, jnp.int32).astype(jnp.float32) - (1.0 + ny / 2)
    shift = jnp.where(row == 0, cell_x, jnp.where(row == 1, cell_y, cell_z))
    return ext + shift


def density_kernel(ext, den_ref, slope_ref, f_ref, acc):
    ex_n, ey_n, _, lanes = ext.shape
    nx, ny = ex_n - 2, ey_n - 2
    slots = 128
    nz = lanes // slots - 2
    dims = (nx, ny, nz)

    def build(index, carry):
        ex, ey = index // ey_n, index % ey_n
        q = centred(ext[ex, ey, 0:3, :], ex, ey, 0, lanes, dims)
        h, m, l = split3(q)
        n = jnp.sum(q * q, axis=0, keepdims=True)
        nh, nm, nl = split3(-n)
        one = jnp.ones((3, lanes), jnp.float32)
        zero = jnp.zeros((KF - 24, lanes), jnp.float32)
        f_ref[index] = jnp.concatenate(
            [2 * h, 2 * m, 2 * h, 2 * l, 2 * h, 2 * m, nh, nm, nl, one, zero], axis=0
        ).astype(jnp.bfloat16)
        return carry

    lax.fori_loop(0, ex_n * ey_n, build, 0)

    def cell(index, carry):
        ix = index // (ny * nz)
        iy = (index // nz) % ny
        iz = index % nz
        start = pl.multiple_of(iz * slots, slots)
        own = ext[ix + 1, iy + 1, :, pl.ds(start + slots, slots)]
        left = own_features(own, ix, iy, iz, dims)
        acc[...] = jnp.zeros_like(acc)
        for dx in range(3):
            for dy in range(3):
                wide = pl.ds(start, 3 * slots)
                d = mm(left, f_ref[(ix + dx) * ey_n + iy + dy, :, wide])
                coef = ext[ix + dx, iy + dy, 3:4, wide]
                w = jnp.maximum(d, 0.0)
                term = w * w * w * coef
                acc[...] += term[:, :slots] + term[:, slots : 2 * slots] + term[:, 2 * slots :]
        total = jnp.sum(acc[...].T, axis=0, keepdims=True)
        alive = own[5:6]
        density = (total - own[3:4]) * alive
        den_ref[ix, iy, pl.ds(iz, 1), :] = density
        slope_ref[ix, iy, :, pl.ds(start, slots)] = (
            -own[6:7] * alive / (2.0 * jnp.sqrt(1.0 + density))
        )
        return carry

    lax.fori_loop(0, nx * ny * nz, cell, 0)


def own_features(own, ix, iy, iz, dims):
    slots = own.shape[1]
    q = centred(own[0:3], ix + 1, iy + 1, iz + 1, slots, dims)
    h, m, l = split3(q)
    nh, nm, nl = split3(1.0 - jnp.sum(q * q, axis=0, keepdims=True))
    one = jnp.ones((3, slots), jnp.float32)
    zero = jnp.zeros((slots - 24, slots), jnp.float32)
    rows = jnp.concatenate([h, h, m, h, l, m, one, nh, nm, nl, zero], axis=0)
    return rows.T[:, :KF].astype(jnp.bfloat16)


def force_kernel(ext, slope, f_ref, out_ref, rows_ref, acc, mine):
    ex_n, ey_n, _, lanes = ext.shape
    nx, ny = ex_n - 2, ey_n - 2
    slots = 128
    nz = lanes // slots - 2
    dims = (nx, ny, nz)

    def build(index, carry):
        ex, ey = index // ey_n, index % ey_n
        block = ext[ex, ey]
        q = centred(block[0:3], ex, ey, 0, lanes, dims)
        c = block[3:4]
        inv = jnp.where(c > 0.0, 1.0 / jnp.where(c > 0.0, c, 1.0), 0.0)
        rho = block[4:5] * inv
        t = -6.0 * slope[ex, ey] * inv
        rows_ref[index] = jnp.concatenate([c * q, c, rho, t, jnp.zeros((2, lanes), jnp.float32)], 0)
        return carry

    lax.fori_loop(0, ex_n * ey_n, build, 0)

    def cell(index, carry):
        ix = index // (ny * nz)
        iy = (index // nz) % ny
        iz = index % nz
        start = pl.multiple_of(iz * slots, slots)
        own = ext[ix + 1, iy + 1, :, pl.ds(start + slots, slots)]
        left = own_features(own, ix, iy, iz, dims)
        own_rows = rows_ref[(ix + 1) * ey_n + iy + 1, :, pl.ds(start + slots, slots)]
        rho = jnp.broadcast_to(-4.0 * own_rows[4:5], (slots, slots))
        mine[0] = rho.T
        mine[1] = jnp.broadcast_to(own_rows[5:6], (slots, slots)).T
        acc[...] = jnp.zeros_like(acc)
        for dx in range(3):
            for dy in range(3):
                row = (ix + dx) * ey_n + iy + dy
                wide = pl.ds(start, 3 * slots)
                d = mm(left, f_ref[row, :, wide])
                near = rows_ref[row, :, wide]
                for part in range(4):
                    size = slots // 4
                    at = slice(part * size, (part + 1) * size)
                    r_i = mine[0, at]
                    t_i = mine[1, at]
                    sums = [jnp.zeros((size, slots), jnp.float32) for _ in range(4)]
                    for k in range(3):
                        lane = slice(k * slots, (k + 1) * slots)
                        w = jnp.maximum(d[at, lane], 0.0)
                        value = w * (r_i * near[4:5, lane] + w * (t_i + near[5:6, lane]))
                        for a in range(4):
                            sums[a] = sums[a] + value * near[a : a + 1, lane]
                    for a in range(4):
                        acc[a, at] += sums[a]
        total = [jnp.sum(acc[a].T, axis=0, keepdims=True) for a in range(4)]
        q = centred(own[0:3], ix + 1, iy + 1, iz + 1, slots, dims)
        out_ref[ix, iy, iz] = own[3:4] * (jnp.concatenate(total[:3], axis=0) - q * total[3])
        return carry

    lax.fori_loop(0, nx * ny * nz, cell, 0)


def hartley(length):
    index = np.arange(length)
    phase = (np.outer(index, index) % length) * (2.0 * np.pi / length)
    return (np.cos(phase) + np.sin(phase)) / np.sqrt(length)


def halves(values):
    high = values.astype(np.float32).astype(jnp.bfloat16)
    low = (values - high.astype(np.float64)).astype(np.float32).astype(jnp.bfloat16)
    return jnp.asarray(high), jnp.asarray(low)


def call(kernel, out_shape, args, scalars=(), scratch=(), flops=1000000):
    specs = [SM if i in scalars else VM for i in range(len(args))]
    outs = jax.tree.map(lambda _: VM, out_shape)
    return pl.pallas_call(
        kernel,
        out_shape=out_shape,
        in_specs=specs,
        out_specs=outs,
        scratch_shapes=list(scratch),
        compiler_params=pltpu.CompilerParams(vmem_limit_bytes=48 * 1024 * 1024),
        cost_estimate=pl.CostEstimate(flops=flops, bytes_accessed=2000000, transcendentals=0),
    )(*args)


def on_device(cell_counts, grid_offset, fraction, species, t_den, t_pair, t_emb, t_chg):
    f32 = jnp.float32
    nx, ny, nz, _, slots = fraction.shape
    gx, gy, gz = (lax.axis_size(a) for a in ("gx", "gy", "gz"))
    every = ("gx", "gy", "gz")
    n_dev = gx * gy * gz
    lx, ly, lz = gx * nx * PPC, gy * ny * PPC, gz * nz * PPC
    xs = nx * PPC
    lanes = ny * nz * PPC
    ys = PPC // gx
    modes = lx // n_dev
    counts = cell_counts.reshape(-1)

    sds = jax.ShapeDtypeStruct
    charge, packed = call(
        spread_kernel,
        (sds((PPC, xs, lanes), f32), sds((nx, ny, 8, nz * slots), f32)),
        (counts, grid_offset, fraction, species, t_den, t_pair, t_emb, t_chg),
        scalars=(0, 4, 5, 6, 7),
    )
    sides = (("gz", 3), ("gy", 1), ("gx", 0))
    ext = padded(packed, sides, (slots, 1, 1))

    qh, ql = halves(hartley(lx))
    zmat = hartley(lz)
    cut = nz * PPC
    wide = np.zeros((gz, ny, cut, ny, lz))
    for c in range(ny):
        wide[:, c, :, c, :] = zmat.reshape(gz, cut, lz)
    wh, wl = halves(wide.reshape(gz * lanes, ny * lz))
    order = (
        np.arange(ly).reshape(gy, ny, gx, ys).transpose(1, 2, 0, 3).reshape(-1)
    )
    kron = np.kron(hartley(ly)[np.ix_(order, order)], np.eye(modes))
    kh, kl = halves(kron)

    def wave(index, length):
        return np.minimum(index, length - index) * (2.0 * math.pi / length)

    wave_y = np.repeat(wave(order, ly), modes).astype(np.float32)[:, None]
    wave_z = wave(np.arange(lz), lz).astype(np.float32)[None, :]
    mode_x = lax.axis_index(every) * modes + jnp.asarray(
        np.tile(np.arange(modes, dtype=np.int32), ly)[:, None]
    )
    wave_x = jnp.minimum(mode_x, lx - mode_x).astype(f32) * (2.0 * math.pi / lx)
    square = wave_x * wave_x + wave_y * wave_y + wave_z * wave_z
    anchor = square == 0.0
    green = jnp.where(
        anchor,
        0.0,
        4.0
        * math.pi
        * jnp.exp(-square / (4.0 * EWALD_SPLIT * EWALD_SPLIT))
        / jnp.where(anchor, 1.0, square),
    )

    direct = modes % 8 == 0
    got = lax.all_to_all(charge.reshape(gx, ys * xs, lanes), "gx", 0, 0, tiled=True)
    got = got.reshape(gx, ys, xs, lanes)
    import functools

    mid = sds((n_dev, ys, modes, lanes) if direct else (ys, lx, lanes), f32)
    modal = call(functools.partial(xmodes_kernel, direct), mid, (got, qh, ql))
    if not direct:
        modal = modal.reshape(ys, n_dev, modes, lanes).transpose(1, 0, 2, 3)
    modal = lax.all_to_all(modal.reshape(n_dev, ys * modes, lanes), every, 0, 0, tiled=True)

    density, slope, feats = call(
        density_kernel,
        (
            sds((nx, ny, nz, slots), f32),
            sds((nx, ny, 1, nz * slots), f32),
            sds(((nx + 2) * (ny + 2), KF, (nz + 2) * slots), jnp.bfloat16),
        ),
        (ext,),
        scratch=(pltpu.VMEM((slots, slots), f32),),
        flops=400000000,
    )
    ext_slope = padded(slope, sides, (slots, 1, 1))

    planes = call(
        plane_kernel,
        sds((gx * gy, gz, ys * modes, lanes), f32),
        (modal.reshape(gx * gy, gz, ys * modes, lanes), wh, wl, kh, kl, green),
    )
    back = lax.all_to_all(planes.reshape(n_dev, ys * modes, lanes), every, 0, 0, tiled=True)
    back = back.reshape(n_dev, ys, modes, lanes)
    if not direct:
        back = back.transpose(1, 0, 2, 3).reshape(ys, lx, lanes)
    lines = call(
        functools.partial(xback_kernel, direct), sds((gx, ys, xs, lanes), f32), (back, qh, ql)
    )
    eam = call(
        force_kernel,
        sds((nx, ny, nz, 3, slots), f32),
        (ext, ext_slope, feats),
        scratch=(
            pltpu.VMEM(((nx + 2) * (ny + 2), 8, (nz + 2) * slots), f32),
            pltpu.VMEM((4, slots, slots), f32),
            pltpu.VMEM((2, slots, slots), f32),
        ),
        flops=800000000,
    )
    phi = lax.all_to_all(lines.reshape(gx, ys * xs, lanes), "gx", 0, 0, tiled=True)
    forces = call(
        sample_kernel,
        sds((nx, ny, nz, 3, slots), f32),
        (counts, grid_offset, fraction, species, t_chg, phi.reshape(PPC, xs, lanes), eam),
        scalars=(0, 4),
    )
    return (forces, density)


def solution(mesh):
    return jax.shard_map(
        on_device,
        mesh=mesh,
        in_specs=(
            P("gx", "gy", "gz"),
            P("gx", "gy", "gz", None, None),
            P("gx", "gy", "gz", None, None),
            P("gx", "gy", "gz", None),
            P(),
            P(),
            P(),
            P(),
        ),
        out_specs=(P("gx", "gy", "gz", None, None), P("gx", "gy", "gz", None)),
        check_vma=False,
    )
```

```python
import functools
import math

import jax
import jax.numpy as jnp
import numpy as np
from jax import lax
from jax.experimental import pallas as pl
from jax.experimental.pallas import tpu as pltpu
from jax.sharding import PartitionSpec as P

PPC = 16
EWALD_SPLIT = 0.7
COUPLING = 8.0
KF = 32
NT = (((1,), (1,)), ((), ()))
NN = (((1,), (0,)), ((), ()))
VM = pl.BlockSpec(memory_space=pltpu.VMEM)
SM = pl.BlockSpec(memory_space=pltpu.SMEM)


def exchange(mesh_sizes, spread, *refs):
    gx, gy, gz = mesh_sizes
    if spread:
        pk, ch, ext, got, send, recv, a_send, a_recv, local = refs
    else:
        pk, ext, send, recv, local = refs
    mx, my, mz = (lax.axis_index(a) for a in ("gx", "gy", "gz"))
    nx, ny, _, lanes = pk.shape
    dirs = [
        (x, y, z) for x in (-1, 0, 1) for y in (-1, 0, 1) for z in (-1, 0, 1) if x or y or z
    ]
    peers = {(x % gx, y % gy, z % gz) for x, y, z in dirs}
    if spread:
        peers |= {(p, 0, 0) for p in range(1, gx)}

    def at(x, y, z):
        return {
            "gx": lax.rem(mx + (x % gx), gx),
            "gy": lax.rem(my + (y % gy), gy),
            "gz": lax.rem(mz + (z % gz), gz),
        }

    barrier = pltpu.get_barrier_semaphore()
    for peer in sorted(peers):
        pl.semaphore_signal(
            barrier, inc=1, device_id=at(*peer), device_id_type=pl.DeviceIdType.MESH
        )
    pl.semaphore_wait(barrier, len(peers))

    copies = []
    if spread:
        for p in range(1, gx):
            target = at(p, 0, 0)
            copies.append(
                pltpu.make_async_remote_copy(
                    src_ref=ch.at[target["gx"]],
                    dst_ref=got.at[mx],
                    send_sem=a_send.at[p - 1],
                    recv_sem=a_recv.at[p - 1],
                    device_id=target,
                    device_id_type=pl.DeviceIdType.MESH,
                )
            )

    def cut(step, count):
        if step == 0:
            return pl.ds(0, count), pl.ds(1, count)
        if step > 0:
            return pl.ds(count - 1, 1), pl.ds(0, 1)
        return pl.ds(0, 1), pl.ds(count + 1, 1)

    def cut_lanes(step):
        if step == 0:
            return pl.ds(0, lanes), pl.ds(128, lanes)
        if step > 0:
            return pl.ds(lanes - 128, 128), pl.ds(0, 128)
        return pl.ds(0, 128), pl.ds(lanes + 128, 128)

    for index, (x, y, z) in enumerate(dirs):
        from_x, to_x = cut(x, nx)
        from_y, to_y = cut(y, ny)
        from_z, to_z = cut_lanes(z)
        copies.append(
            pltpu.make_async_remote_copy(
                src_ref=pk.at[from_x, from_y, :, from_z],
                dst_ref=ext.at[to_x, to_y, :, to_z],
                send_sem=send.at[index],
                recv_sem=recv.at[index],
                device_id=at(x, y, z),
                device_id_type=pl.DeviceIdType.MESH,
            )
        )
    copies.append(
        pltpu.make_async_copy(
            pk, ext.at[pl.ds(1, nx), pl.ds(1, ny), :, pl.ds(128, lanes)], local.at[0]
        )
    )
    if spread:
        copies.append(pltpu.make_async_copy(ch.at[mx], got.at[mx], local.at[1]))
    for copy in copies:
        copy.start()
    for copy in copies:
        copy.wait()


def split2(values):
    high = values.astype(jnp.bfloat16)
    low = (values - high.astype(jnp.float32)).astype(jnp.bfloat16)
    return high, low


def split3(values):
    high = values.astype(jnp.bfloat16).astype(jnp.float32)
    rest = values - high
    mid = rest.astype(jnp.bfloat16).astype(jnp.float32)
    low = (rest - mid).astype(jnp.bfloat16).astype(jnp.float32)
    return high, mid, low


def mm(a, b, dims=NN):
    return lax.dot_general(a, b, dims, preferred_element_type=jnp.float32)


def mm3(a, b, dims=NN):
    return mm(a[0], b[0], dims) + mm(a[0], b[1], dims) + mm(a[1], b[0], dims)


def mm6(a, b, dims=NN):
    small = mm(a[0], b[2], dims) + mm(a[2], b[0], dims) + mm(a[1], b[1], dims)
    return mm(a[0], b[0], dims) + (mm(a[0], b[1], dims) + (mm(a[1], b[0], dims) + small))


def parts3(values):
    return [part.astype(jnp.bfloat16) for part in split3(values)]


def table(sp, ref, which):
    result = jnp.zeros(sp.shape, jnp.float32)
    kinds = ref.shape[0] // 4
    for kind in range(kinds):
        result = jnp.where(sp == kind, ref[which * kinds + kind], result)
    return result


def weights_of(off, fr):
    points = lax.broadcasted_iota(jnp.int32, (PPC, off.shape[1]), 0)
    lower = points == off
    upper = points == off + 1
    zero = jnp.zeros((PPC, off.shape[1]), jnp.float32)
    weights = jnp.where(lower, 1.0 - fr, jnp.where(upper, fr, zero))
    slopes = jnp.where(lower, -1.0, jnp.where(upper, 1.0, zero))
    return weights, slopes


def placed(rows, cell, cells):
    parts = []
    if cell:
        parts.append(jnp.zeros((cell * PPC, rows.shape[1]), jnp.float32))
    parts.append(rows)
    if cell < cells - 1:
        parts.append(jnp.zeros(((cells - 1 - cell) * PPC, rows.shape[1]), jnp.float32))
    return jnp.concatenate(parts, axis=0)


def spread_kernel(cnt, off, fr, sp, tab, s_ref, pk_ref):
    nx, ny, _, nz, slots = fr.shape

    def body(cx, carry):
        total = jnp.zeros((PPC * PPC, ny * nz * PPC), jnp.float32)
        for cy in range(ny):
            for cz in range(nz):
                cell = cy * nz + cz
                o = jnp.concatenate([off[cx, cy, d, cz : cz + 1, :] for d in range(3)], axis=0)
                f = jnp.concatenate([fr[cx, cy, d, cz : cz + 1, :] for d in range(3)], axis=0)
                kind = sp[cx, cy, cz : cz + 1, :]
                lane = lax.broadcasted_iota(jnp.int32, (1, slots), 1)
                alive = (lane < cnt[(cx * ny + cy) * nz + cz]).astype(jnp.float32)
                charge = table(kind, tab, 3) * alive
                pos = (o.astype(jnp.float32) + 0.5 + f) / PPC
                zero = jnp.zeros((1, slots), jnp.float32)
                pk_ref[cx, cy, :, cz * slots : (cz + 1) * slots] = jnp.concatenate(
                    [
                        pos,
                        table(kind, tab, 0) * alive,
                        table(kind, tab, 1) * alive,
                        alive,
                        table(kind, tab, 2),
                        zero,
                    ],
                    axis=0,
                )
                wx, _ = weights_of(o[0:1], f[0:1])
                wy, _ = weights_of(o[1:2], f[1:2])
                wz, _ = weights_of(o[2:3], f[2:3])
                wx = wx * charge
                plane = (wy[:, None, :] * wx[None, :, :]).reshape(PPC * PPC, slots)
                ph, pw = split2(plane)
                zh, zw = split2(placed(wz, cell, ny * nz))
                total = total + mm(
                    jnp.concatenate([ph, pw], axis=1), jnp.concatenate([zh, zh], axis=1), NT
                )
                total = total + mm(ph, zw, NT)
        s_ref[:, pl.ds(pl.multiple_of(cx * PPC, PPC), PPC), :] = total.reshape(
            PPC, PPC, ny * nz * PPC
        )
        return carry

    lax.fori_loop(0, nx, body, 0)


def xmodes_kernel(direct, r_ref, q_ref, h_ref):
    gx, ys, xs, lanes = r_ref.shape
    q = split2(q_ref[...])
    for y in range(ys):
        data = r_ref[:, y].reshape(gx * xs, lanes)
        out = mm3(q, split2(data))
        if direct:
            h_ref[:, y] = out.reshape(h_ref.shape[0], h_ref.shape[2], lanes)
        else:
            h_ref[y] = out


def xback_kernel(direct, h_ref, q_ref, p_ref):
    gx, ys, xs, lanes = p_ref.shape
    q = parts3(q_ref[...])
    for y in range(ys):
        data = h_ref[:, y].reshape(gx * xs, lanes) if direct else h_ref[y]
        out = mm6(q, parts3(data))
        p_ref[:, y] = out.reshape(gx, xs, lanes)


def plane_kernel(t_ref, z_ref, k_ref, green, o_ref):
    groups, gz, sub, lanes = t_ref.shape
    rows = groups * sub
    lz = green.shape[1]
    cut = lz // gz
    ny = lanes // cut
    q = z_ref[...]
    blocks = []
    for g in range(gz):
        for c in range(ny):
            pieces = [jnp.zeros((cut, lz), jnp.float32)] * ny
            pieces[c] = q[g * cut : (g + 1) * cut]
            blocks.append(jnp.concatenate(pieces, axis=1))
    w = parts3(jnp.concatenate(blocks, axis=0))
    k = parts3(k_ref[...])
    data = jnp.concatenate([t_ref[:, g].reshape(rows, lanes) for g in range(gz)], axis=1)
    u = mm3(split2(data), w)
    u = jnp.concatenate([u[:, c * lz : (c + 1) * lz] for c in range(ny)], axis=0)
    v = mm3(k, split2(u)) * green[...]
    u = mm6(k, parts3(v))
    u = jnp.concatenate([u[c * rows : (c + 1) * rows] for c in range(ny)], axis=1)
    out = mm6(parts3(u), w, NT)
    for g in range(gz):
        o_ref[:, g] = out[:, g * lanes : (g + 1) * lanes].reshape(groups, sub, lanes)


def rest_of(low, right):
    top = jnp.concatenate([low, jnp.zeros_like(low)], axis=1)
    return jnp.concatenate([top, right], axis=0)


def sample_kernel(cnt, off, fr, sp, tab, phi_ref, eam_a, eam_b, out_ref):
    nx, ny, _, nz, slots = fr.shape

    def body(cx, carry, eam, first):
        phi = phi_ref[:, pl.ds(pl.multiple_of(cx * PPC, PPC), PPC), :].reshape(
            PPC * PPC, ny * nz * PPC
        )
        ph, pw, pl3 = parts3(phi)
        both = jnp.concatenate([ph, pw], axis=1)
        for cy in range(ny):
            for cz in range(nz):
                cell = cy * nz + cz
                o = jnp.concatenate([off[cx, cy, d, cz : cz + 1, :] for d in range(3)], axis=0)
                f = jnp.concatenate([fr[cx, cy, d, cz : cz + 1, :] for d in range(3)], axis=0)
                kind = sp[cx, cy, cz : cz + 1, :]
                lane = lax.broadcasted_iota(jnp.int32, (1, slots), 1)
                alive = (lane < cnt[(cx * ny + cy) * nz + cz]).astype(jnp.float32)
                charge = table(kind, tab, 3) * alive
                wx, sx = weights_of(o[0:1], f[0:1])
                wy, sy = weights_of(o[1:2], f[1:2])
                wz, sz = weights_of(o[2:3], f[2:3])
                zh, zw = split2(placed(wz, cell, ny * nz))
                sh = placed(sz, cell, ny * nz).astype(jnp.bfloat16)
                right = jnp.concatenate([zh, sh], axis=1)
                g = mm(both, jnp.concatenate([right, right], axis=0))
                more = mm(jnp.concatenate([ph, pl3], axis=1), rest_of(zw, right))
                gw = g[:, :slots] + more[:, :slots]
                gs = g[:, slots:] + more[:, slots:]
                fx = jnp.zeros((PPC, slots), jnp.float32)
                fy = jnp.zeros((PPC, slots), jnp.float32)
                fz = jnp.zeros((PPC, slots), jnp.float32)
                for y in range(PPC):
                    a = gw[y * PPC : (y + 1) * PPC]
                    b = gs[y * PPC : (y + 1) * PPC]
                    fx = fx + wy[y : y + 1] * a
                    fy = fy + sy[y : y + 1] * a
                    fz = fz + wy[y : y + 1] * b
                field = jnp.concatenate(
                    [
                        jnp.sum(sx * fx, axis=0, keepdims=True),
                        jnp.sum(wx * fy, axis=0, keepdims=True),
                        jnp.sum(wx * fz, axis=0, keepdims=True),
                    ],
                    axis=0,
                )
                out = (eam[cx - first, cy, cz] - COUPLING * charge * field) * alive
                for d in range(3):
                    out_ref[cx, cy, d, cz : cz + 1, :] = out[d : d + 1]
        return carry

    half = eam_a.shape[0]
    lax.fori_loop(0, half, lambda cx, c: body(cx, c, eam_a, 0), 0)
    lax.fori_loop(half, nx, lambda cx, c: body(cx, c, eam_b, half), 0)


def centred(ext, ex, ey, first_z, lanes, dims):
    nx, ny, nz = dims
    slots_iota = lax.broadcasted_iota(jnp.int32, (3, lanes), 1)
    row = lax.broadcasted_iota(jnp.int32, (3, lanes), 0)
    cell_z = (slots_iota // 128).astype(jnp.float32) + (
        jnp.asarray(first_z, jnp.int32).astype(jnp.float32) - (1.0 + nz / 2)
    )
    cell_x = jnp.asarray(ex, jnp.int32).astype(jnp.float32) - (1.0 + nx / 2)
    cell_y = jnp.asarray(ey, jnp.int32).astype(jnp.float32) - (1.0 + ny / 2)
    shift = jnp.where(row == 0, cell_x, jnp.where(row == 1, cell_y, cell_z))
    return ext + shift


def density_kernel(ext, den_ref, slope_ref, f_ref, acc):
    ex_n, ey_n, _, lanes = ext.shape
    nx, ny = ex_n - 2, ey_n - 2
    slots = 128
    nz = lanes // slots - 2
    dims = (nx, ny, nz)

    def build(index, carry):
        ex, ey = index // ey_n, index % ey_n
        q = centred(ext[ex, ey, 0:3, :], ex, ey, 0, lanes, dims)
        h, m, l = split3(q)
        n = jnp.sum(q * q, axis=0, keepdims=True)
        nh, nm, nl = split3(-n)
        one = jnp.ones((3, lanes), jnp.float32)
        zero = jnp.zeros((KF - 24, lanes), jnp.float32)
        f_ref[index] = jnp.concatenate(
            [2 * h, 2 * m, 2 * h, 2 * l, 2 * h, 2 * m, nh, nm, nl, one, zero], axis=0
        ).astype(jnp.bfloat16)
        return carry

    lax.fori_loop(0, ex_n * ey_n, build, 0)

    def cell(index, carry):
        ix = index // (ny * nz)
        iy = (index // nz) % ny
        iz = index % nz
        start = pl.multiple_of(iz * slots, slots)
        own = ext[ix + 1, iy + 1, :, pl.ds(start + slots, slots)]
        left = own_features(own, ix, iy, iz, dims)
        acc[...] = jnp.zeros_like(acc)
        for dx in range(3):
            for dy in range(3):
                wide = pl.ds(start, 3 * slots)
                d = mm(left, f_ref[(ix + dx) * ey_n + iy + dy, :, wide])
                coef = ext[ix + dx, iy + dy, 3:4, wide]
                w = jnp.maximum(d, 0.0)
                term = w * w * w * coef
                acc[...] += term[:, :slots] + term[:, slots : 2 * slots] + term[:, 2 * slots :]
        total = jnp.sum(acc[...].T, axis=0, keepdims=True)
        alive = own[5:6]
        density = (total - own[3:4]) * alive
        den_ref[ix, iy, pl.ds(iz, 1), :] = density
        slope_ref[ix, iy, :, pl.ds(start, slots)] = (
            -own[6:7] * alive / (2.0 * jnp.sqrt(1.0 + density))
        )
        return carry

    lax.fori_loop(0, nx * ny * nz, cell, 0)


def own_features(own, ix, iy, iz, dims):
    slots = own.shape[1]
    q = centred(own[0:3], ix + 1, iy + 1, iz + 1, slots, dims)
    h, m, l = split3(q)
    nh, nm, nl = split3(1.0 - jnp.sum(q * q, axis=0, keepdims=True))
    one = jnp.ones((3, slots), jnp.float32)
    zero = jnp.zeros((slots - 24, slots), jnp.float32)
    rows = jnp.concatenate([h, h, m, h, l, m, one, nh, nm, nl, zero], axis=0)
    return rows.T[:, :KF].astype(jnp.bfloat16)


def force_kernel(first, *refs):
    if first == 0:
        ext, slope, f_ref, out_ref, rows_ref, acc, mine = refs
    else:
        ext, rows_ref, f_ref, out_ref, acc, mine = refs
    ex_n, ey_n, _, lanes = ext.shape
    nx, ny = ex_n - 2, ey_n - 2
    slots = 128
    nz = lanes // slots - 2
    dims = (nx, ny, nz)

    def build(index, carry):
        ex, ey = index // ey_n, index % ey_n
        block = ext[ex, ey]
        q = centred(block[0:3], ex, ey, 0, lanes, dims)
        c = block[3:4]
        inv = jnp.where(c > 0.0, 1.0 / jnp.where(c > 0.0, c, 1.0), 0.0)
        rho = block[4:5] * inv
        t = -6.0 * slope[ex, ey] * inv
        rows_ref[index] = jnp.concatenate([c * q, c, rho, t, jnp.zeros((2, lanes), jnp.float32)], 0)
        return carry

    if first == 0:
        lax.fori_loop(0, ex_n * ey_n, build, 0)

    def cell(index, carry):
        ix = index // (ny * nz)
        iy = (index // nz) % ny
        iz = index % nz
        start = pl.multiple_of(iz * slots, slots)
        own = ext[ix + 1, iy + 1, :, pl.ds(start + slots, slots)]
        left = own_features(own, ix, iy, iz, dims)
        own_rows = rows_ref[(ix + 1) * ey_n + iy + 1, :, pl.ds(start + slots, slots)]
        rho = jnp.broadcast_to(-4.0 * own_rows[4:5], (slots, slots))
        mine[0] = rho.T
        mine[1] = jnp.broadcast_to(own_rows[5:6], (slots, slots)).T
        acc[...] = jnp.zeros_like(acc)
        for dx in range(3):
            for dy in range(3):
                row = (ix + dx) * ey_n + iy + dy
                wide = pl.ds(start, 3 * slots)
                d = mm(left, f_ref[row, :, wide])
                near = rows_ref[row, :, wide]
                for part in range(4):
                    size = slots // 4
                    at = slice(part * size, (part + 1) * size)
                    r_i = mine[0, at]
                    t_i = mine[1, at]
                    sums = [jnp.zeros((size, slots), jnp.float32) for _ in range(4)]
                    for k in range(3):
                        lane = slice(k * slots, (k + 1) * slots)
                        w = jnp.maximum(d[at, lane], 0.0)
                        value = w * (r_i * near[4:5, lane] + w * (t_i + near[5:6, lane]))
                        for a in range(4):
                            sums[a] = sums[a] + value * near[a : a + 1, lane]
                    for a in range(4):
                        acc[a, at] += sums[a]
        total = [jnp.sum(acc[a].T, axis=0, keepdims=True) for a in range(4)]
        q = centred(own[0:3], ix + 1, iy + 1, iz + 1, slots, dims)
        out_ref[ix - first, iy, iz] = own[3:4] * (jnp.concatenate(total[:3], axis=0) - q * total[3])
        return carry

    begin = first * ny * nz
    lax.fori_loop(begin, begin + out_ref.shape[0] * ny * nz, cell, 0)


def hartley(length):
    index = np.arange(length)
    phase = (np.outer(index, index) % length) * (2.0 * np.pi / length)
    return (np.cos(phase) + np.sin(phase)) / np.sqrt(length)


def call(kernel, out_shape, args, scalars=(), scratch=(), flops=1000000, collective=None):
    specs = [SM if i in scalars else VM for i in range(len(args))]
    outs = jax.tree.map(lambda _: VM, out_shape)
    return pl.pallas_call(
        kernel,
        out_shape=out_shape,
        in_specs=specs,
        out_specs=outs,
        scratch_shapes=list(scratch),
        compiler_params=pltpu.CompilerParams(
            vmem_limit_bytes=48 * 1024 * 1024,
            collective_id=collective,
            has_side_effects=collective is not None,
        ),
        cost_estimate=pl.CostEstimate(flops=flops, bytes_accessed=2000000, transcendentals=0),
    )(*args)


def on_device(cell_counts, grid_offset, fraction, species, t_den, t_pair, t_emb, t_chg):
    f32 = jnp.float32
    nx, ny, nz, _, slots = fraction.shape
    gx, gy, gz = (lax.axis_size(a) for a in ("gx", "gy", "gz"))
    every = ("gx", "gy", "gz")
    n_dev = gx * gy * gz
    lx, ly, lz = gx * nx * PPC, gy * ny * PPC, gz * nz * PPC
    xs = nx * PPC
    lanes = ny * nz * PPC
    ys = PPC // gx
    modes = lx // n_dev
    counts = cell_counts.reshape(-1)

    sds = jax.ShapeDtypeStruct
    tables = jnp.concatenate([t_den, t_pair, t_emb, t_chg])
    offs = grid_offset.transpose(0, 1, 3, 2, 4)
    fracs = fraction.transpose(0, 1, 3, 2, 4)
    atoms = (counts, offs, fracs, species, tables)
    charge, packed = call(
        spread_kernel,
        (sds((PPC, xs, lanes), f32), sds((nx, ny, 8, nz * slots), f32)),
        atoms,
        scalars=(0, 4),
    )
    dma = pltpu.SemaphoreType.DMA
    sizes = (gx, gy, gz)
    ext, got = call(
        functools.partial(exchange, sizes, True),
        (
            sds((nx + 2, ny + 2, 8, (nz + 2) * slots), f32),
            sds((gx, ys * xs, lanes), f32),
        ),
        (packed, charge.reshape(gx, ys * xs, lanes)),
        scratch=(dma((26,)), dma((26,)), dma((gx - 1,)), dma((gx - 1,)), dma((2,))),
        collective=0,
    )

    q_x = jnp.asarray(hartley(lx).astype(np.float32))
    q_z = q_x if lx == lz else jnp.asarray(hartley(lz).astype(np.float32))
    order = (
        np.arange(ly).reshape(gy, ny, gx, ys).transpose(1, 2, 0, 3).reshape(-1)
    )
    kron = np.kron(hartley(ly)[np.ix_(order, order)], np.eye(modes))
    q_y = jnp.asarray(kron.astype(np.float32))

    def wave(index, length):
        return np.minimum(index, length - index) * (2.0 * math.pi / length)

    wave_y = np.repeat(wave(order, ly), modes).astype(np.float32)[:, None]
    wave_z = wave(np.arange(lz), lz).astype(np.float32)[None, :]
    mode_x = lax.axis_index(every) * modes + jnp.asarray(
        np.tile(np.arange(modes, dtype=np.int32), ly)[:, None]
    )
    wave_x = jnp.minimum(mode_x, lx - mode_x).astype(f32) * (2.0 * math.pi / lx)
    square = wave_x * wave_x + wave_y * wave_y + wave_z * wave_z
    anchor = square == 0.0
    green = jnp.where(
        anchor,
        0.0,
        4.0
        * math.pi
        * jnp.exp(-square / (4.0 * EWALD_SPLIT * EWALD_SPLIT))
        / jnp.where(anchor, 1.0, square),
    )

    direct = modes % 8 == 0
    got = got.reshape(gx, ys, xs, lanes)
    mid = sds((n_dev, ys, modes, lanes) if direct else (ys, lx, lanes), f32)
    modal = call(functools.partial(xmodes_kernel, direct), mid, (got, q_x))
    if not direct:
        modal = modal.reshape(ys, n_dev, modes, lanes).transpose(1, 0, 2, 3)
    ext, modal = lax.optimization_barrier((ext, modal))
    modal = lax.all_to_all(modal.reshape(n_dev, ys * modes, lanes), every, 0, 0, tiled=True)

    density, slope, feats = call(
        density_kernel,
        (
            sds((nx, ny, nz, slots), f32),
            sds((nx, ny, 1, nz * slots), f32),
            sds(((nx + 2) * (ny + 2), KF, (nz + 2) * slots), jnp.bfloat16),
        ),
        (ext,),
        scratch=(pltpu.VMEM((slots, slots), f32),),
        flops=400000000,
    )
    green, slope = lax.optimization_barrier((green, slope))

    planes = call(
        plane_kernel,
        sds((gx * gy, gz, ys * modes, lanes), f32),
        (modal.reshape(gx * gy, gz, ys * modes, lanes), q_z, q_y, green),
    )
    planes, slope = lax.optimization_barrier((planes, slope))
    back = lax.all_to_all(planes.reshape(n_dev, ys * modes, lanes), every, 0, 0, tiled=True)
    ext_slope = call(
        functools.partial(exchange, sizes, False),
        sds((nx + 2, ny + 2, 1, (nz + 2) * slots), f32),
        (slope,),
        scratch=(dma((26,)), dma((26,)), dma((1,))),
        collective=1,
    )
    half = max(nx // 2, 1)
    scratch = (pltpu.VMEM((4, slots, slots), f32), pltpu.VMEM((2, slots, slots), f32))
    eam_a, rows = call(
        functools.partial(force_kernel, 0),
        (
            sds((half, ny, nz, 3, slots), f32),
            sds(((nx + 2) * (ny + 2), 8, (nz + 2) * slots), f32),
        ),
        (ext, ext_slope, feats),
        scratch=scratch,
        flops=400000000,
    )
    q_back, rows = lax.optimization_barrier((q_x, rows))
    back = back.reshape(n_dev, ys, modes, lanes)
    if not direct:
        back = back.transpose(1, 0, 2, 3).reshape(ys, lx, lanes)
    lines = call(
        functools.partial(xback_kernel, direct), sds((gx, ys, xs, lanes), f32), (back, q_back)
    )
    lines, rows = lax.optimization_barrier((lines, rows))
    phi = lax.all_to_all(lines.reshape(gx, ys * xs, lanes), "gx", 0, 0, tiled=True)
    eam_b = call(
        functools.partial(force_kernel, half),
        sds((nx - half, ny, nz, 3, slots), f32),
        (ext, rows, feats),
        scratch=scratch,
        flops=400000000,
    )
    forces = call(
        sample_kernel,
        sds((nx, ny, 3, nz, slots), f32),
        atoms + (phi.reshape(PPC, xs, lanes), eam_a, eam_b),
        scalars=(0, 4),
    )
    return (forces.transpose(0, 1, 3, 2, 4), density)


def solution(mesh):
    return jax.shard_map(
        on_device,
        mesh=mesh,
        in_specs=(
            P("gx", "gy", "gz"),
            P("gx", "gy", "gz", None, None),
            P("gx", "gy", "gz", None, None),
            P("gx", "gy", "gz", None),
            P(),
            P(),
            P(),
            P(),
        ),
        out_specs=(P("gx", "gy", "gz", None, None), P("gx", "gy", "gz", None)),
        check_vma=False,
    )
```

```python
import functools
import math

import jax
import jax.numpy as jnp
import numpy as np
from jax import lax
from jax.experimental import pallas as pl
from jax.experimental.pallas import tpu as pltpu
from jax.sharding import PartitionSpec as P

PPC = 16
EWALD_SPLIT = 0.7
COUPLING = 8.0
KF = 32
NT = (((1,), (1,)), ((), ()))
NN = (((1,), (0,)), ((), ()))
VM = pl.BlockSpec(memory_space=pltpu.VMEM)
SM = pl.BlockSpec(memory_space=pltpu.SMEM)


def exchange(mesh_sizes, spread, *refs):
    gx, gy, gz = mesh_sizes
    if spread:
        pk, ch, ext, got, send, recv, a_send, a_recv, local = refs
    else:
        pk, ext, send, recv, local = refs
    mx, my, mz = (lax.axis_index(a) for a in ("gx", "gy", "gz"))
    nx, ny, _, lanes = pk.shape
    dirs = [
        (x, y, z) for x in (-1, 0, 1) for y in (-1, 0, 1) for z in (-1, 0, 1) if x or y or z
    ]
    peers = {(x % gx, y % gy, z % gz) for x, y, z in dirs}
    if spread:
        peers |= {(p, 0, 0) for p in range(1, gx)}

    def at(x, y, z):
        return {
            "gx": lax.rem(mx + (x % gx), gx),
            "gy": lax.rem(my + (y % gy), gy),
            "gz": lax.rem(mz + (z % gz), gz),
        }

    barrier = pltpu.get_barrier_semaphore()
    for peer in sorted(peers):
        pl.semaphore_signal(
            barrier, inc=1, device_id=at(*peer), device_id_type=pl.DeviceIdType.MESH
        )
    pl.semaphore_wait(barrier, len(peers))

    copies = []
    if spread:
        for p in range(1, gx):
            target = at(p, 0, 0)
            copies.append(
                pltpu.make_async_remote_copy(
                    src_ref=ch.at[target["gx"]],
                    dst_ref=got.at[mx],
                    send_sem=a_send.at[p - 1],
                    recv_sem=a_recv.at[p - 1],
                    device_id=target,
                    device_id_type=pl.DeviceIdType.MESH,
                )
            )

    def cut(step, count):
        if step == 0:
            return pl.ds(0, count), pl.ds(1, count)
        if step > 0:
            return pl.ds(count - 1, 1), pl.ds(0, 1)
        return pl.ds(0, 1), pl.ds(count + 1, 1)

    def cut_lanes(step):
        if step == 0:
            return pl.ds(0, lanes), pl.ds(128, lanes)
        if step > 0:
            return pl.ds(lanes - 128, 128), pl.ds(0, 128)
        return pl.ds(0, 128), pl.ds(lanes + 128, 128)

    for index, (x, y, z) in enumerate(dirs):
        from_x, to_x = cut(x, nx)
        from_y, to_y = cut(y, ny)
        from_z, to_z = cut_lanes(z)
        copies.append(
            pltpu.make_async_remote_copy(
                src_ref=pk.at[from_x, from_y, :, from_z],
                dst_ref=ext.at[to_x, to_y, :, to_z],
                send_sem=send.at[index],
                recv_sem=recv.at[index],
                device_id=at(x, y, z),
                device_id_type=pl.DeviceIdType.MESH,
            )
        )
    copies.append(
        pltpu.make_async_copy(
            pk, ext.at[pl.ds(1, nx), pl.ds(1, ny), :, pl.ds(128, lanes)], local.at[0]
        )
    )
    if spread:
        copies.append(pltpu.make_async_copy(ch.at[mx], got.at[mx], local.at[1]))
    for copy in copies:
        copy.start()
    for copy in copies:
        copy.wait()


def split2(values):
    high = values.astype(jnp.bfloat16)
    low = (values - high.astype(jnp.float32)).astype(jnp.bfloat16)
    return high, low


def split3(values):
    high = values.astype(jnp.bfloat16).astype(jnp.float32)
    rest = values - high
    mid = rest.astype(jnp.bfloat16).astype(jnp.float32)
    low = (rest - mid).astype(jnp.bfloat16).astype(jnp.float32)
    return high, mid, low


def mm(a, b, dims=NN):
    return lax.dot_general(a, b, dims, preferred_element_type=jnp.float32)


def mm3(a, b, dims=NN):
    return mm(a[0], b[0], dims) + mm(a[0], b[1], dims) + mm(a[1], b[0], dims)


def mm6(a, b, dims=NN):
    small = mm(a[0], b[2], dims) + mm(a[2], b[0], dims) + mm(a[1], b[1], dims)
    return mm(a[0], b[0], dims) + (mm(a[0], b[1], dims) + (mm(a[1], b[0], dims) + small))


def parts3(values):
    return [part.astype(jnp.bfloat16) for part in split3(values)]


def table(sp, ref, which):
    result = jnp.zeros(sp.shape, jnp.float32)
    kinds = ref.shape[0] // 4
    for kind in range(kinds):
        result = jnp.where(sp == kind, ref[which * kinds + kind], result)
    return result


def weights_of(off, fr):
    points = lax.broadcasted_iota(jnp.int32, (PPC, off.shape[1]), 0)
    lower = points == off
    upper = points == off + 1
    zero = jnp.zeros((PPC, off.shape[1]), jnp.float32)
    weights = jnp.where(lower, 1.0 - fr, jnp.where(upper, fr, zero))
    slopes = jnp.where(lower, -1.0, jnp.where(upper, 1.0, zero))
    return weights, slopes


def placed(rows, cell, cells):
    parts = []
    if cell:
        parts.append(jnp.zeros((cell * PPC, rows.shape[1]), jnp.float32))
    parts.append(rows)
    if cell < cells - 1:
        parts.append(jnp.zeros(((cells - 1 - cell) * PPC, rows.shape[1]), jnp.float32))
    return jnp.concatenate(parts, axis=0)


def spread_kernel(cnt, off, fr, sp, tab, s_ref, pk_ref):
    nx, ny, _, nz, slots = fr.shape

    def body(cx, carry):
        total = jnp.zeros((PPC * PPC, ny * nz * PPC), jnp.float32)
        for cy in range(ny):
            for cz in range(nz):
                cell = cy * nz + cz
                o = jnp.concatenate([off[cx, cy, d, cz : cz + 1, :] for d in range(3)], axis=0)
                f = jnp.concatenate([fr[cx, cy, d, cz : cz + 1, :] for d in range(3)], axis=0)
                kind = sp[cx, cy, cz : cz + 1, :]
                lane = lax.broadcasted_iota(jnp.int32, (1, slots), 1)
                alive = (lane < cnt[(cx * ny + cy) * nz + cz]).astype(jnp.float32)
                charge = table(kind, tab, 3) * alive
                pos = (o.astype(jnp.float32) + 0.5 + f) / PPC
                zero = jnp.zeros((1, slots), jnp.float32)
                pk_ref[cx, cy, :, cz * slots : (cz + 1) * slots] = jnp.concatenate(
                    [
                        pos,
                        table(kind, tab, 0) * alive,
                        table(kind, tab, 1) * alive,
                        alive,
                        table(kind, tab, 2),
                        zero,
                    ],
                    axis=0,
                )
                wx, _ = weights_of(o[0:1], f[0:1])
                wy, _ = weights_of(o[1:2], f[1:2])
                wz, _ = weights_of(o[2:3], f[2:3])
                wx = wx * charge
                plane = (wy[:, None, :] * wx[None, :, :]).reshape(PPC * PPC, slots)
                ph, pw = split2(plane)
                zh, zw = split2(placed(wz, cell, ny * nz))
                total = total + mm(
                    jnp.concatenate([ph, pw], axis=1), jnp.concatenate([zh, zh], axis=1), NT
                )
                total = total + mm(ph, zw, NT)
        s_ref[:, pl.ds(pl.multiple_of(cx * PPC, PPC), PPC), :] = total.reshape(
            PPC, PPC, ny * nz * PPC
        )
        return carry

    lax.fori_loop(0, nx, body, 0)


def xmodes_kernel(direct, r_ref, q_ref, h_ref):
    gx, ys, xs, lanes = r_ref.shape
    q = split2(q_ref[...])
    for y in range(ys):
        data = r_ref[:, y].reshape(gx * xs, lanes)
        out = mm3(q, split2(data))
        if direct:
            h_ref[:, y] = out.reshape(h_ref.shape[0], h_ref.shape[2], lanes)
        else:
            h_ref[y] = out


def xback_kernel(direct, h_ref, q_ref, p_ref):
    gx, ys, xs, lanes = p_ref.shape
    q = parts3(q_ref[...])
    for y in range(ys):
        data = h_ref[:, y].reshape(gx * xs, lanes) if direct else h_ref[y]
        out = mm6(q, parts3(data))
        p_ref[:, y] = out.reshape(gx, xs, lanes)


def plane_kernel(t_ref, z_ref, k_ref, green, o_ref):
    groups, gz, sub, lanes = t_ref.shape
    rows = groups * sub
    lz = green.shape[1]
    cut = lz // gz
    ny = lanes // cut
    q = z_ref[...]
    blocks = []
    for g in range(gz):
        for c in range(ny):
            pieces = [jnp.zeros((cut, lz), jnp.float32)] * ny
            pieces[c] = q[g * cut : (g + 1) * cut]
            blocks.append(jnp.concatenate(pieces, axis=1))
    w = parts3(jnp.concatenate(blocks, axis=0))
    k = parts3(k_ref[...])
    data = jnp.concatenate([t_ref[:, g].reshape(rows, lanes) for g in range(gz)], axis=1)
    u = mm3(split2(data), w)
    u = jnp.concatenate([u[:, c * lz : (c + 1) * lz] for c in range(ny)], axis=0)
    v = mm3(k, split2(u)) * green[...]
    u = mm6(k, parts3(v))
    u = jnp.concatenate([u[c * rows : (c + 1) * rows] for c in range(ny)], axis=1)
    out = mm6(parts3(u), w, NT)
    for g in range(gz):
        o_ref[:, g] = out[:, g * lanes : (g + 1) * lanes].reshape(groups, sub, lanes)


def rest_of(low, right):
    top = jnp.concatenate([low, jnp.zeros_like(low)], axis=1)
    return jnp.concatenate([top, right], axis=0)


def sample_kernel(cnt, off, fr, sp, tab, phi_ref, eam_a, eam_b, eam_c, out_ref):
    nx, ny, _, nz, slots = fr.shape

    def body(cx, carry, eam, first):
        phi = phi_ref[:, pl.ds(pl.multiple_of(cx * PPC, PPC), PPC), :].reshape(
            PPC * PPC, ny * nz * PPC
        )
        ph, pw, pl3 = parts3(phi)
        both = jnp.concatenate([ph, pw], axis=1)
        for cy in range(ny):
            for cz in range(nz):
                cell = cy * nz + cz
                o = jnp.concatenate([off[cx, cy, d, cz : cz + 1, :] for d in range(3)], axis=0)
                f = jnp.concatenate([fr[cx, cy, d, cz : cz + 1, :] for d in range(3)], axis=0)
                kind = sp[cx, cy, cz : cz + 1, :]
                lane = lax.broadcasted_iota(jnp.int32, (1, slots), 1)
                alive = (lane < cnt[(cx * ny + cy) * nz + cz]).astype(jnp.float32)
                charge = table(kind, tab, 3) * alive
                wx, sx = weights_of(o[0:1], f[0:1])
                wy, sy = weights_of(o[1:2], f[1:2])
                wz, sz = weights_of(o[2:3], f[2:3])
                zh, zw = split2(placed(wz, cell, ny * nz))
                sh = placed(sz, cell, ny * nz).astype(jnp.bfloat16)
                right = jnp.concatenate([zh, sh], axis=1)
                g = mm(both, jnp.concatenate([right, right], axis=0))
                more = mm(jnp.concatenate([ph, pl3], axis=1), rest_of(zw, right))
                gw = g[:, :slots] + more[:, :slots]
                gs = g[:, slots:] + more[:, slots:]
                fx = jnp.zeros((PPC, slots), jnp.float32)
                fy = jnp.zeros((PPC, slots), jnp.float32)
                fz = jnp.zeros((PPC, slots), jnp.float32)
                for y in range(PPC):
                    a = gw[y * PPC : (y + 1) * PPC]
                    b = gs[y * PPC : (y + 1) * PPC]
                    fx = fx + wy[y : y + 1] * a
                    fy = fy + sy[y : y + 1] * a
                    fz = fz + wy[y : y + 1] * b
                field = jnp.concatenate(
                    [
                        jnp.sum(sx * fx, axis=0, keepdims=True),
                        jnp.sum(wx * fy, axis=0, keepdims=True),
                        jnp.sum(wx * fz, axis=0, keepdims=True),
                    ],
                    axis=0,
                )
                out = (eam[cx - first, cy, cz] - COUPLING * charge * field) * alive
                for d in range(3):
                    out_ref[cx, cy, d, cz : cz + 1, :] = out[d : d + 1]
        return carry

    half = eam_a.shape[0]
    lax.fori_loop(0, half, lambda cx, c: body(cx, c, eam_a, 0), 0)
    lax.fori_loop(half, 2 * half, lambda cx, c: body(cx, c, eam_b, half), 0)
    lax.fori_loop(2 * half, nx, lambda cx, c: body(cx, c, eam_c, 2 * half), 0)


def centred(ext, ex, ey, first_z, lanes, dims):
    nx, ny, nz = dims
    slots_iota = lax.broadcasted_iota(jnp.int32, (3, lanes), 1)
    row = lax.broadcasted_iota(jnp.int32, (3, lanes), 0)
    cell_z = (slots_iota // 128).astype(jnp.float32) + (
        jnp.asarray(first_z, jnp.int32).astype(jnp.float32) - (1.0 + nz / 2)
    )
    cell_x = jnp.asarray(ex, jnp.int32).astype(jnp.float32) - (1.0 + nx / 2)
    cell_y = jnp.asarray(ey, jnp.int32).astype(jnp.float32) - (1.0 + ny / 2)
    shift = jnp.where(row == 0, cell_x, jnp.where(row == 1, cell_y, cell_z))
    return ext + shift


def density_kernel(ext, den_ref, slope_ref, f_ref, acc):
    ex_n, ey_n, _, lanes = ext.shape
    nx, ny = ex_n - 2, ey_n - 2
    slots = 128
    nz = lanes // slots - 2
    dims = (nx, ny, nz)

    def build(index, carry):
        ex, ey = index // ey_n, index % ey_n
        q = centred(ext[ex, ey, 0:3, :], ex, ey, 0, lanes, dims)
        h, m, l = split3(q)
        n = jnp.sum(q * q, axis=0, keepdims=True)
        nh, nm, nl = split3(-n)
        one = jnp.ones((3, lanes), jnp.float32)
        zero = jnp.zeros((KF - 24, lanes), jnp.float32)
        f_ref[index] = jnp.concatenate(
            [2 * h, 2 * m, 2 * h, 2 * l, 2 * h, 2 * m, nh, nm, nl, one, zero], axis=0
        ).astype(jnp.bfloat16)
        return carry

    lax.fori_loop(0, ex_n * ey_n, build, 0)

    def cell(index, carry):
        ix = index // (ny * nz)
        iy = (index // nz) % ny
        iz = index % nz
        start = pl.multiple_of(iz * slots, slots)
        own = ext[ix + 1, iy + 1, :, pl.ds(start + slots, slots)]
        left = own_features(own, ix, iy, iz, dims)
        acc[...] = jnp.zeros_like(acc)
        for dx in range(3):
            for dy in range(3):
                wide = pl.ds(start, 3 * slots)
                d = mm(left, f_ref[(ix + dx) * ey_n + iy + dy, :, wide])
                coef = ext[ix + dx, iy + dy, 3:4, wide]
                w = jnp.maximum(d, 0.0)
                term = w * w * w * coef
                acc[...] += term[:, :slots] + term[:, slots : 2 * slots] + term[:, 2 * slots :]
        total = jnp.sum(acc[...].T, axis=0, keepdims=True)
        alive = own[5:6]
        density = (total - own[3:4]) * alive
        den_ref[ix, iy, pl.ds(iz, 1), :] = density
        slope_ref[ix, iy, :, pl.ds(start, slots)] = (
            -own[6:7] * alive / (2.0 * jnp.sqrt(1.0 + density))
        )
        return carry

    lax.fori_loop(0, nx * ny * nz, cell, 0)


def own_features(own, ix, iy, iz, dims):
    slots = own.shape[1]
    q = centred(own[0:3], ix + 1, iy + 1, iz + 1, slots, dims)
    h, m, l = split3(q)
    nh, nm, nl = split3(1.0 - jnp.sum(q * q, axis=0, keepdims=True))
    one = jnp.ones((3, slots), jnp.float32)
    zero = jnp.zeros((slots - 24, slots), jnp.float32)
    rows = jnp.concatenate([h, h, m, h, l, m, one, nh, nm, nl, zero], axis=0)
    return rows.T[:, :KF].astype(jnp.bfloat16)


def force_kernel(first, *refs):
    if first == 0:
        ext, slope, f_ref, out_ref, rows_ref, acc, mine = refs
    else:
        ext, rows_ref, f_ref, out_ref, acc, mine = refs
    ex_n, ey_n, _, lanes = ext.shape
    nx, ny = ex_n - 2, ey_n - 2
    slots = 128
    nz = lanes // slots - 2
    dims = (nx, ny, nz)

    def build(index, carry):
        ex, ey = index // ey_n, index % ey_n
        block = ext[ex, ey]
        q = centred(block[0:3], ex, ey, 0, lanes, dims)
        c = block[3:4]
        inv = jnp.where(c > 0.0, 1.0 / jnp.where(c > 0.0, c, 1.0), 0.0)
        rho = block[4:5] * inv
        t = -6.0 * slope[ex, ey] * inv
        rows_ref[index] = jnp.concatenate([c * q, c, rho, t, jnp.zeros((2, lanes), jnp.float32)], 0)
        return carry

    if first == 0:
        lax.fori_loop(0, ex_n * ey_n, build, 0)

    def cell(index, carry):
        ix = index // (ny * nz)
        iy = (index // nz) % ny
        iz = index % nz
        start = pl.multiple_of(iz * slots, slots)
        own = ext[ix + 1, iy + 1, :, pl.ds(start + slots, slots)]
        left = own_features(own, ix, iy, iz, dims)
        own_rows = rows_ref[(ix + 1) * ey_n + iy + 1, :, pl.ds(start + slots, slots)]
        rho = jnp.broadcast_to(-4.0 * own_rows[4:5], (slots, slots))
        mine[0] = rho.T
        mine[1] = jnp.broadcast_to(own_rows[5:6], (slots, slots)).T
        acc[...] = jnp.zeros_like(acc)
        for dx in range(3):
            for dy in range(3):
                row = (ix + dx) * ey_n + iy + dy
                wide = pl.ds(start, 3 * slots)
                d = mm(left, f_ref[row, :, wide])
                near = rows_ref[row, :, wide]
                for part in range(4):
                    size = slots // 4
                    at = slice(part * size, (part + 1) * size)
                    r_i = mine[0, at]
                    t_i = mine[1, at]
                    sums = [jnp.zeros((size, slots), jnp.float32) for _ in range(4)]
                    for k in range(3):
                        lane = slice(k * slots, (k + 1) * slots)
                        w = jnp.maximum(d[at, lane], 0.0)
                        value = w * (r_i * near[4:5, lane] + w * (t_i + near[5:6, lane]))
                        for a in range(4):
                            sums[a] = sums[a] + value * near[a : a + 1, lane]
                    for a in range(4):
                        acc[a, at] += sums[a]
        total = [jnp.sum(acc[a].T, axis=0, keepdims=True) for a in range(4)]
        q = centred(own[0:3], ix + 1, iy + 1, iz + 1, slots, dims)
        out_ref[ix - first, iy, iz] = own[3:4] * (jnp.concatenate(total[:3], axis=0) - q * total[3])
        return carry

    begin = first * ny * nz
    lax.fori_loop(begin, begin + out_ref.shape[0] * ny * nz, cell, 0)


def hartley(length):
    index = np.arange(length)
    phase = (np.outer(index, index) % length) * (2.0 * np.pi / length)
    return (np.cos(phase) + np.sin(phase)) / np.sqrt(length)


def call(kernel, out_shape, args, scalars=(), scratch=(), flops=1000000, collective=None):
    specs = [SM if i in scalars else VM for i in range(len(args))]
    outs = jax.tree.map(lambda _: VM, out_shape)
    return pl.pallas_call(
        kernel,
        out_shape=out_shape,
        in_specs=specs,
        out_specs=outs,
        scratch_shapes=list(scratch),
        compiler_params=pltpu.CompilerParams(
            vmem_limit_bytes=48 * 1024 * 1024,
            collective_id=collective,
            has_side_effects=collective is not None,
        ),
        cost_estimate=pl.CostEstimate(flops=flops, bytes_accessed=2000000, transcendentals=0),
    )(*args)


def on_device(cell_counts, grid_offset, fraction, species, t_den, t_pair, t_emb, t_chg):
    f32 = jnp.float32
    nx, ny, nz, _, slots = fraction.shape
    gx, gy, gz = (lax.axis_size(a) for a in ("gx", "gy", "gz"))
    every = ("gx", "gy", "gz")
    n_dev = gx * gy * gz
    lx, ly, lz = gx * nx * PPC, gy * ny * PPC, gz * nz * PPC
    xs = nx * PPC
    lanes = ny * nz * PPC
    ys = PPC // gx
    modes = lx // n_dev
    counts = cell_counts.reshape(-1)

    sds = jax.ShapeDtypeStruct
    tables = jnp.concatenate([t_den, t_pair, t_emb, t_chg])
    offs = grid_offset.transpose(0, 1, 3, 2, 4)
    fracs = fraction.transpose(0, 1, 3, 2, 4)
    atoms = (counts, offs, fracs, species, tables)
    charge, packed = call(
        spread_kernel,
        (sds((PPC, xs, lanes), f32), sds((nx, ny, 8, nz * slots), f32)),
        atoms,
        scalars=(0, 4),
    )
    dma = pltpu.SemaphoreType.DMA
    sizes = (gx, gy, gz)
    ext = call(
        functools.partial(exchange, sizes, False),
        sds((nx + 2, ny + 2, 8, (nz + 2) * slots), f32),
        (packed,),
        scratch=(dma((26,)), dma((26,)), dma((1,))),
        collective=0,
    )
    charge, ext = lax.optimization_barrier((charge, ext))
    got = lax.all_to_all(charge.reshape(gx, ys * xs, lanes), "gx", 0, 0, tiled=True)

    q_x = jnp.asarray(hartley(lx).astype(np.float32))
    q_z = q_x if lx == lz else jnp.asarray(hartley(lz).astype(np.float32))
    order = (
        np.arange(ly).reshape(gy, ny, gx, ys).transpose(1, 2, 0, 3).reshape(-1)
    )
    kron = np.kron(hartley(ly)[np.ix_(order, order)], np.eye(modes))
    q_y = jnp.asarray(kron.astype(np.float32))

    def wave(index, length):
        return np.minimum(index, length - index) * (2.0 * math.pi / length)

    wave_y = np.repeat(wave(order, ly), modes).astype(np.float32)[:, None]
    wave_z = wave(np.arange(lz), lz).astype(np.float32)[None, :]
    mode_x = lax.axis_index(every) * modes + jnp.asarray(
        np.tile(np.arange(modes, dtype=np.int32), ly)[:, None]
    )
    wave_x = jnp.minimum(mode_x, lx - mode_x).astype(f32) * (2.0 * math.pi / lx)
    square = wave_x * wave_x + wave_y * wave_y + wave_z * wave_z
    anchor = square == 0.0
    green = jnp.where(
        anchor,
        0.0,
        4.0
        * math.pi
        * jnp.exp(-square / (4.0 * EWALD_SPLIT * EWALD_SPLIT))
        / jnp.where(anchor, 1.0, square),
    )

    density, slope, feats = call(
        density_kernel,
        (
            sds((nx, ny, nz, slots), f32),
            sds((nx, ny, 1, nz * slots), f32),
            sds(((nx + 2) * (ny + 2), KF, (nz + 2) * slots), jnp.bfloat16),
        ),
        (ext,),
        scratch=(pltpu.VMEM((slots, slots), f32),),
        flops=400000000,
    )
    q_first, slope = lax.optimization_barrier((q_x, slope))
    ext_slope = call(
        functools.partial(exchange, sizes, False),
        sds((nx + 2, ny + 2, 1, (nz + 2) * slots), f32),
        (slope,),
        scratch=(dma((26,)), dma((26,)), dma((1,))),
        collective=1,
    )

    direct = modes % 8 == 0
    got = got.reshape(gx, ys, xs, lanes)
    mid = sds((n_dev, ys, modes, lanes) if direct else (ys, lx, lanes), f32)
    modal = call(functools.partial(xmodes_kernel, direct), mid, (got, q_first))
    if not direct:
        modal = modal.reshape(ys, n_dev, modes, lanes).transpose(1, 0, 2, 3)
    ext_slope, modal = lax.optimization_barrier((ext_slope, modal))
    modal = lax.all_to_all(modal.reshape(n_dev, ys * modes, lanes), every, 0, 0, tiled=True)

    half = max(nx // 4, 1)
    scratch = (pltpu.VMEM((4, slots, slots), f32), pltpu.VMEM((2, slots, slots), f32))
    eam_a, rows = call(
        functools.partial(force_kernel, 0),
        (
            sds((half, ny, nz, 3, slots), f32),
            sds(((nx + 2) * (ny + 2), 8, (nz + 2) * slots), f32),
        ),
        (ext, ext_slope, feats),
        scratch=scratch,
        flops=400000000,
    )
    green, rows = lax.optimization_barrier((green, rows))

    planes = call(
        plane_kernel,
        sds((gx * gy, gz, ys * modes, lanes), f32),
        (modal.reshape(gx * gy, gz, ys * modes, lanes), q_z, q_y, green),
    )
    planes, rows = lax.optimization_barrier((planes, rows))
    back = lax.all_to_all(planes.reshape(n_dev, ys * modes, lanes), every, 0, 0, tiled=True)
    eam_b = call(
        functools.partial(force_kernel, half),
        sds((half, ny, nz, 3, slots), f32),
        (ext, rows, feats),
        scratch=scratch,
        flops=200000000,
    )
    q_back, eam_b = lax.optimization_barrier((q_x, eam_b))
    back = back.reshape(n_dev, ys, modes, lanes)
    if not direct:
        back = back.transpose(1, 0, 2, 3).reshape(ys, lx, lanes)
    lines = call(
        functools.partial(xback_kernel, direct), sds((gx, ys, xs, lanes), f32), (back, q_back)
    )
    lines, rows = lax.optimization_barrier((lines, rows))
    phi = lax.all_to_all(lines.reshape(gx, ys * xs, lanes), "gx", 0, 0, tiled=True)
    eam_c = call(
        functools.partial(force_kernel, 2 * half),
        sds((nx - 2 * half, ny, nz, 3, slots), f32),
        (ext, rows, feats),
        scratch=scratch,
        flops=400000000,
    )
    forces = call(
        sample_kernel,
        sds((nx, ny, 3, nz, slots), f32),
        atoms + (phi.reshape(PPC, xs, lanes), eam_a, eam_b, eam_c),
        scalars=(0, 4),
    )
    return (forces.transpose(0, 1, 3, 2, 4), density)


def solution(mesh):
    return jax.shard_map(
        on_device,
        mesh=mesh,
        in_specs=(
            P("gx", "gy", "gz"),
            P("gx", "gy", "gz", None, None),
            P("gx", "gy", "gz", None, None),
            P("gx", "gy", "gz", None),
            P(),
            P(),
            P(),
            P(),
        ),
        out_specs=(P("gx", "gy", "gz", None, None), P("gx", "gy", "gz", None)),
        check_vma=False,
    )
```
